256 devices in a mesh: grp: 32 (over z, x_lo, core), patch: 8 (over y, x_hi).
Axes of the slice: x: 4 (x_hi: 2, x_lo: 2; x = x_hi * 2 + x_lo), y: 4, z: 8, core: 2. Of those that a mesh axis runs over, the one named last changes fastest.
Arguments:
- tokens: bfloat16 [98304, 1152], P(('grp', 'patch')), parts along dimension 0, may hold values from -6 to 6
- projection_weight: bfloat16 [1152, 3456], replicated, may hold values from -0.1875 to 0.1875
- shift_term: float32 [1152], replicated, may hold values from -3 to 3
- scale_term: float32 [1152], replicated, may hold values from -3 to 3
- query_gain: float32 [72], replicated, may hold values from 0.1 to 1.9
- key_gain: float32 [72], replicated, may hold values from 0.1 to 1.9
- stale_keys: bfloat16 [98304, 1152], P(('grp', 'patch')), parts along dimension 0, may hold values from -6 to 6
- stale_values: bfloat16 [98304, 1152], P(('grp', 'patch')), parts along dimension 0, may hold values from -6 to 6
- stale_output: bfloat16 [98304, 1152], P(('grp', 'patch')), parts along dimension 0, may hold values from -3 to 3
- refreshed: int32 [6144], P('grp'), parts along dimension 0, may hold values from 0 to 1, as said below
Outputs:
- attended: bfloat16 [98304, 1152], P(('grp', 'patch')), parts along dimension 0
The draws below stay inside these ranges and needn't reach their ends.
There are 32 independent parts, one for each index of `grp`. The reference program is written for one: setup_inputs(seed, part) draws one part's arguments, and reference() takes and returns one part's arrays. A program takes and returns all parts, laid end to end along the dimension named above; an argument that names none is the same for every part. Nothing has to cross between parts.
Inputs may be any that keep to these rules, and one draw needn't show every extreme that they name: Exactly 64 of the 192 entries are 1; in every prompt some device has all 24 of its tiles refreshed.
All inputs are finite; a program needn't handle non-finite values.
Results may differ from the reference program's by a relative error of at most 0.0045.
Values may be sent and summed in bfloat16 or wider, within the bound.
A program may use at most 128 MiB of HBM per device.

```python
import math
import jax
import jax.numpy as jnp
from jax import lax

D = 1152
H = 16
HD = 72
TILE = 16
TILES_DEV = 24
TOKENS = 3072
TILES = 192
REFRESHED = 64


def draw_refreshed(key, part):
    heavy_key = jax.random.fold_in(key, 11)
    order_key = jax.random.fold_in(key, 12)
    heavy = jax.random.randint(heavy_key, (), 0, TILES // TILES_DEV)
    ordering = jax.random.permutation(order_key, TILES).astype(jnp.int32)
    holder = jnp.arange(TILES, dtype=jnp.int32) // TILES_DEV
    scores = ordering + jnp.where(holder == heavy, TILES, 0).astype(jnp.int32)
    leading = jnp.argsort(-scores, stable=True)[:REFRESHED]
    return jnp.zeros((TILES,), jnp.int32).at[leading].set(1)


def block_levels(own_key, dims, cuts, low, largest):
    factor_of = 1.0
    for dim, shards_of in cuts:
        heights = jax.random.uniform(jax.random.fold_in(jax.random.fold_in(own_key, 6), dim), (shards_of,), jnp.float32, low / len(cuts), largest / len(cuts))
        factor_of = factor_of * jnp.repeat(jnp.exp(heights), dims[dim] // shards_of).reshape((-1,) + (1,) * (len(dims) - 1 - dim))
    return factor_of


def noise(own_key, dims, deviation, most, pieces=(), kind=jnp.bfloat16):
    factor_of = block_levels(own_key, dims, pieces, -0.22, 0.18) if pieces else 1.0
    result = jax.random.normal(own_key, dims, jnp.float32) * deviation * factor_of
    return jnp.minimum(jnp.maximum(result, -most), most).astype(kind)


def setup_inputs(seed: int = 0, part: int = 0) -> dict:
    arg_keys = jax.random.split(jax.random.key(seed), 11)
    part_splits = jax.random.split(jax.random.fold_in(arg_keys[10], part), 11)
    return {
        "tokens": noise(part_splits[0], (TOKENS, D), 1.0, 6.0, ((0, 8),)),
        "projection_weight": noise(arg_keys[1], (D, 3 * D), D ** -0.5, 0.1875),
        "shift_term": noise(arg_keys[2], (D,), 0.5, 3.0, (), jnp.float32),
        "scale_term": noise(arg_keys[3], (D,), 0.5, 3.0, (), jnp.float32),
        "query_gain": jnp.clip(1.0 + 0.18 * jax.random.normal(arg_keys[4], (HD,), jnp.float32), 0.1, 1.9),
        "key_gain": jnp.clip(1.0 + 0.18 * jax.random.normal(arg_keys[5], (HD,), jnp.float32), 0.1, 1.9),
        "stale_keys": noise(part_splits[6], (TOKENS, D), 1.0, 6.0, ((0, 8),)),
        "stale_values": noise(part_splits[7], (TOKENS, D), 1.0, 6.0, ((0, 8),)),
        "stale_output": noise(part_splits[8], (TOKENS, D), 0.5, 3.0, ((0, 8),)),
        "refreshed": draw_refreshed(jax.random.fold_in(jax.random.fold_in(arg_keys[10], part), 71), part),
    }


epsilon = 1e-06

def modulate(row_block, shift_term, scale_term):
    values = row_block.astype(jnp.float32)
    center = values - lax.optimization_barrier(jnp.mean(values, axis=-1, keepdims=True))
    spread = lax.optimization_barrier(jnp.mean(center * center, axis=-1, keepdims=True))
    normed = center / jnp.sqrt(spread + epsilon)
    return (normed * (1.0 + scale_term) + shift_term).astype(jnp.bfloat16)

def head_norm(row_block, gain_vector, head_count):
    values = row_block.astype(jnp.float32).reshape(row_block.shape[0], head_count, -1)
    normed = values / jnp.sqrt(lax.optimization_barrier(jnp.mean(values * values, axis=-1, keepdims=True)) + epsilon)
    return (normed * gain_vector).astype(jnp.bfloat16).reshape(row_block.shape[0], -1)

def reference(tokens, projection_weight, shift_term, scale_term, query_gain, key_gain, stale_keys, stale_values, stale_output, refreshed):
    model_width = tokens.shape[1]
    row_mask = jnp.repeat(refreshed, TILE) > 0
    hidden = modulate(tokens, shift_term, scale_term)
    projected = jnp.dot(hidden, projection_weight, preferred_element_type=jnp.float32)
    query_new = projected[:, :model_width].astype(jnp.bfloat16)
    key_new = projected[:, model_width:2 * model_width].astype(jnp.bfloat16)
    value_new = projected[:, 2 * model_width:].astype(jnp.bfloat16)
    keys_all = jnp.where(row_mask[:, None], key_new, stale_keys)
    values_all = jnp.where(row_mask[:, None], value_new, stale_values)
    key_normed = head_norm(keys_all, key_gain, H)
    query_normed = head_norm(query_new, query_gain, H)
    chosen = jnp.nonzero(row_mask, size=REFRESHED * TILE, fill_value=0)[0].astype(jnp.int32)
    selected = query_normed[chosen]
    factor = 1.0 / math.sqrt(HD)
    query_heads = selected.reshape(-1, H, HD).transpose(1, 0, 2)
    key_heads = key_normed.reshape(-1, H, HD).transpose(1, 0, 2)
    value_heads = values_all.reshape(-1, H, HD).transpose(1, 0, 2)

    def per_head(operands):
        query_one, key_one, value_one = operands
        scores = jnp.dot(query_one.astype(jnp.float32), key_one.astype(jnp.float32).T, precision=lax.Precision.HIGHEST) * factor
        weights = jnp.exp(scores)
        totals = lax.optimization_barrier(jnp.sum(weights, axis=1))
        rounded = lax.optimization_barrier(weights.astype(jnp.bfloat16)).astype(jnp.float32)
        numerator = jnp.dot(rounded, value_one.astype(jnp.float32), precision=lax.Precision.HIGHEST)
        return numerator / totals[:, None]
    fresh_heads = lax.map(per_head, (query_heads, key_heads, value_heads))
    fresh_rows = fresh_heads.transpose(1, 0, 2).reshape(-1, model_width).astype(jnp.bfloat16)
    return stale_output.at[chosen].set(fresh_rows)
```

```python
import functools
import math

import jax
import jax.numpy as jnp
from jax import lax
from jax.experimental import pallas as pl
from jax.experimental.pallas import tpu as pltpu
from jax.sharding import PartitionSpec as P

H = 16
HD = 72
TILE = 16
D = H * HD
PARTS = 8
ROWS = 384
TILES_DEV = ROWS // TILE
TILES = PARTS * TILES_DEV
REFRESHED = 64
FRESH = REFRESHED * TILE
HEADS_DEV = H // PARTS
BLOCK = 384
QBLOCK = 256
TOKEN_LOADS = 3
NORM_BLOCK = 64
MESH = pl.DeviceIdType.MESH
EPSILON = 1e-06
F32 = jnp.float32
BF16 = jnp.bfloat16

OFFSETS = ((2, 1), (2, 0), (1, 1), (3, 1), (0, 1), (1, 0), (3, 0))


def dot(a, b):
    return jnp.dot(a, b, preferred_element_type=F32)


def dot_nt(a, b):
    return lax.dot_general(a, b, (((1,), (1,)), ((), ())), preferred_element_type=F32)


def eye(n):
    rows = lax.broadcasted_iota(jnp.int32, (n, n), 0)
    columns = lax.broadcasted_iota(jnp.int32, (n, n), 1)
    return jnp.where(rows == columns, 1.0, 0.0).astype(BF16)


def kernel(
    tokens_hbm,
    weight_hbm,
    shift_ref,
    scale_ref,
    query_gain_ref,
    key_gain_ref,
    stale_keys_hbm,
    stale_values_hbm,
    stale_output_hbm,
    refreshed_ref,
    out_ref,
    tokens,
    weight,
    stale,
    hidden,
    turned,
    own_mask,
    query_send,
    kv_send,
    query_recv,
    kv_recv,
    query_rows,
    query_fresh,
    numerator,
    totals,
    attended,
    out_send,
    out_recv,
    plan_vmem,
    plan,
    load_sem,
    weight_sem,
    stale_sem,
    plan_sem,
    own_sem,
    q_send_sem,
    q_recv_sem,
    kv_send_sem,
    kv_recv_sem,
    o_send_sem,
    o_recv_sem,
):
    grp = lax.axis_index("grp")
    me = lax.axis_index("patch")
    my_y, my_x = me // 2, me % 2

    def target(k):
        dy, dx = OFFSETS[k]
        return lax.rem(my_y + dy, 4) * 2 + lax.rem(my_x + dx, 2)

    def source(k):
        dy, dx = OFFSETS[k]
        return lax.rem(my_y + 4 - dy, 4) * 2 + lax.rem(my_x + dx, 2)

    loads = []
    for part in range(TOKEN_LOADS):
        rows = pl.ds(part * (ROWS // TOKEN_LOADS), ROWS // TOKEN_LOADS)
        loads.append(pltpu.make_async_copy(tokens_hbm.at[rows], tokens.at[rows], load_sem.at[part]))
    weight_loads = []
    for part in range(3):
        columns = pl.ds(part * D, D)
        weight_loads.append(
            pltpu.make_async_copy(weight_hbm.at[:, columns], weight.at[part], weight_sem.at[part])
        )
    stale_loads = []
    for slot, ref in enumerate((stale_keys_hbm, stale_values_hbm, stale_output_hbm)):
        stale_loads.append(pltpu.make_async_copy(ref, stale.at[slot], stale_sem.at[slot]))
    for load in loads:
        load.start()
    for part in range(3):
        weight_loads[part].start()
        stale_loads[part].start()

    barrier = pltpu.get_barrier_semaphore()
    for k in range(PARTS - 1):
        pl.semaphore_signal(barrier, inc=1, device_id=(grp, target(k)), device_id_type=MESH)

    def column(gain_ref):
        same = lax.broadcasted_iota(jnp.int32, (HD, HD), 0) == lax.broadcasted_iota(
            jnp.int32, (HD, HD), 1
        )
        row = jnp.broadcast_to(gain_ref[...].reshape(1, HD), (HD, HD))
        return jnp.sum(jnp.where(same, row, 0.0), axis=1, keepdims=True)

    shift = shift_ref[...].reshape(1, D)
    scale = 1.0 + scale_ref[...].reshape(1, D)
    with jax.named_scope("norm"):
        for part in range(TOKEN_LOADS):
            loads[part].wait()
            for block in range(ROWS // TOKEN_LOADS // NORM_BLOCK):
                rows = pl.ds(part * (ROWS // TOKEN_LOADS) + block * NORM_BLOCK, NORM_BLOCK)
                values = tokens[rows, :].astype(F32)
                center = values - jnp.mean(values, axis=-1, keepdims=True)
                spread = jnp.mean(center * center, axis=-1, keepdims=True)
                normed = center * (1.0 / jnp.sqrt(spread + EPSILON))
                hidden[rows, :] = (normed * scale + shift).astype(BF16)

    def project(part):
        for block in range(D // BLOCK):
            columns = pl.ds(block * BLOCK, BLOCK)
            fresh = dot(hidden[...], weight[part, :, columns]).astype(BF16)
            if part > 0:
                mask = own_mask[...]
                mask = jnp.concatenate([mask] * (BLOCK // 128), axis=1)
                old = stale[part - 1, :, columns].astype(F32)
                fresh = jnp.where(mask > 0.5, fresh.astype(F32), old).astype(BF16)
            turned[columns, :] = fresh.T

    def head_norm(head, gain):
        values = turned[pl.ds(head * HD, HD), :].astype(F32)
        mean = jnp.sum(values * values, axis=0, keepdims=True) * (1.0 / HD)
        return (values * (1.0 / jnp.sqrt(mean + EPSILON)) * gain).astype(BF16)

    with jax.named_scope("proj_q"):
        weight_loads[0].wait()
        project(0)
    with jax.named_scope("norm_q"):
        gain = column(query_gain_ref)
        for head in range(H):
            query_send[head // HEADS_DEV, head % HEADS_DEV] = head_norm(head, gain)
    with jax.named_scope("barrier"):
        pl.semaphore_wait(barrier, PARTS - 1)

    def query_copy(k):
        return pltpu.make_async_remote_copy(
            src_ref=query_send.at[target(k)],
            dst_ref=query_recv.at[me],
            send_sem=q_send_sem.at[k],
            recv_sem=q_recv_sem.at[k],
            device_id=(grp, target(k)),
            device_id_type=MESH,
        )

    def kv_copy(head, k):
        return pltpu.make_async_remote_copy(
            src_ref=kv_send.at[head, target(k)],
            dst_ref=kv_recv.at[head, me],
            send_sem=kv_send_sem.at[head, k],
            recv_sem=kv_recv_sem.at[head, k],
            device_id=(grp, target(k)),
            device_id_type=MESH,
        )

    def out_copy(head, k):
        return pltpu.make_async_remote_copy(
            src_ref=out_send.at[head, target(k)],
            dst_ref=out_recv.at[me, head],
            send_sem=o_send_sem.at[head, k],
            recv_sem=o_recv_sem.at[head, k],
            device_id=(grp, target(k)),
            device_id_type=MESH,
        )

    own_query = pltpu.make_async_copy(query_send.at[me], query_recv.at[me], own_sem.at[0])
    own_kv = [
        pltpu.make_async_copy(kv_send.at[h, me], kv_recv.at[h, me], own_sem.at[1 + h])
        for h in range(HEADS_DEV)
    ]
    own_out = [
        pltpu.make_async_copy(out_send.at[h, me], out_recv.at[me, h], own_sem.at[3 + h])
        for h in range(HEADS_DEV)
    ]
    for k in range(PARTS - 1):
        query_copy(k).start()
    own_query.start()

    flags = refreshed_ref[...].reshape(1, TILES).astype(F32)
    tile_row = lax.broadcasted_iota(jnp.int32, (TILES, TILES), 0)
    tile_col = lax.broadcasted_iota(jnp.int32, (TILES, TILES), 1)
    flag_rows = jnp.broadcast_to(flags, (TILES, TILES))
    until = jnp.where(tile_col <= tile_row, flag_rows, 0.0).astype(BF16)
    inclusive = dot(until, jnp.ones((TILES, 128), BF16))
    slots = lax.broadcasted_iota(jnp.int32, (TILES, 128), 1).astype(F32)
    which = jnp.sum(jnp.where(inclusive <= slots, 1.0, 0.0), axis=0, keepdims=True)
    which = jnp.minimum(which, float(TILES - 1))
    before = jnp.where(tile_row < tile_col, 1.0, 0.0).astype(BF16)
    rank = dot(jnp.broadcast_to(flags, (8, TILES)).astype(BF16), before)[0:1]
    rank = jnp.minimum(rank, float(REFRESHED - 1))
    plan_vmem[0:1, 0:128] = which.astype(jnp.int32)
    plan_vmem[1:2, 0:TILES] = rank.astype(jnp.int32)
    plan_copy = pltpu.make_async_copy(plan_vmem, plan, plan_sem)
    plan_copy.start()
    row_tile = lax.broadcasted_iota(jnp.int32, (ROWS, TILES), 0) // TILE + me * TILES_DEV
    row_col = lax.broadcasted_iota(jnp.int32, (ROWS, TILES), 1)
    chosen = jnp.where(row_tile == row_col, jnp.broadcast_to(flags, (ROWS, TILES)), 0.0)
    own_mask[...] = dot(chosen.astype(BF16), jnp.ones((TILES, 128), BF16))

    with jax.named_scope("proj_k"):
        weight_loads[1].wait()
        stale_loads[0].wait()
        project(1)
    with jax.named_scope("norm_k"):
        gain = column(key_gain_ref)
        for head in range(H):
            kv_send[head % HEADS_DEV, head // HEADS_DEV, 0] = head_norm(head, gain)
    with jax.named_scope("proj_v"):
        weight_loads[2].wait()
        stale_loads[1].wait()
        project(2)
    with jax.named_scope("put_v"):
        for head in range(H):
            kv_send[head % HEADS_DEV, head // HEADS_DEV, 1] = turned[pl.ds(head * HD, HD), :]
    for h in range(HEADS_DEV):
        for k in range(PARTS - 1):
            kv_copy(h, k).start()
        own_kv[h].start()

    numerator[...] = jnp.zeros_like(numerator)
    totals[...] = jnp.zeros_like(totals)
    same = eye(ROWS)

    def turn_queries(index):
        for h in range(HEADS_DEV):
            rows = dot_nt(same, query_recv[index, h]).astype(BF16)
            query_rows[h, pl.ds(index * TILES_DEV, TILES_DEV)] = rows.reshape(TILES_DEV, TILE, HD)

    with jax.named_scope("turn_q"):
        own_query.wait()
        turn_queries(me)
        for k in range(PARTS - 1):
            query_copy(k).wait_recv()
            turn_queries(source(k))
    with jax.named_scope("keep_fresh"):
        plan_copy.wait()
        for slot in range(REFRESHED):
            tile = jnp.clip(plan[0, slot], 0, TILES - 1)
            for h in range(HEADS_DEV):
                query_fresh[h, slot] = query_rows[h, tile]
    factor = math.log2(math.e) / math.sqrt(HD)
    tiles_block = QBLOCK // TILE

    def add_block(head, index):
        keys = kv_recv[head, index, 0]
        values = kv_recv[head, index, 1]

        for block in range(FRESH // QBLOCK):
            rows = pl.ds(block * QBLOCK, QBLOCK)
            queries = query_fresh[head, pl.ds(block * tiles_block, tiles_block)]
            scores = dot(queries.reshape(QBLOCK, HD), keys)
            weights = jnp.exp2(scores * factor)
            sums = weights[:, 0:128]
            for lane in range(128, ROWS, 128):
                sums = sums + weights[:, lane : lane + 128]
            totals[head, rows, :] += sums
            numerator[head, rows, :] += dot_nt(weights.astype(BF16), values)

    def send_out(head):
        for block in range(FRESH // QBLOCK):
            rows = pl.ds(block * QBLOCK, QBLOCK)
            total = jnp.sum(totals[head, rows, :], axis=1, keepdims=True)
            result = (numerator[head, rows, :] / total).astype(BF16)
            attended[head, pl.ds(block * tiles_block, tiles_block)] = result.reshape(
                tiles_block, TILE, HD
            )

        same = eye(HD)
        for owner in range(PARTS):
            pieces = []
            for tile in range(TILES_DEV):
                item = jnp.clip(plan[1, owner * TILES_DEV + tile], 0, REFRESHED - 1)
                pieces.append(attended[head, item])
            rows = jnp.concatenate(pieces, axis=0)
            out_send[head, owner] = dot_nt(same, rows).astype(BF16)
        for k in range(PARTS - 1):
            out_copy(head, k).start()
        own_out[head].start()

    for h in range(HEADS_DEV):
        with jax.named_scope("add_own"):
            own_kv[h].wait()
            add_block(h, me)
        for k in range(PARTS - 1):
            with jax.named_scope(f"wait_kv#h={h}#k={k}"):
                kv_copy(h, k).wait_recv()
            with jax.named_scope("add"):
                add_block(h, source(k))
        with jax.named_scope("send_out"):
            send_out(h)

    with jax.named_scope("wait_out"):
        stale_loads[2].wait()
        for h in range(HEADS_DEV):
            own_out[h].wait()
            for k in range(PARTS - 1):
                out_copy(h, k).wait_recv()
    with jax.named_scope("merge"):
        for owner in range(PARTS):
            for h in range(HEADS_DEV):
                turned[pl.ds((owner * HEADS_DEV + h) * HD, HD), :] = out_recv[owner, h]
        mask = own_mask[...] > 0.5
        for block in range(D // 128):
            columns = pl.ds(block * 128, 128)
            fresh = turned[columns, :].T.astype(F32)
            out_ref[:, columns] = jnp.where(mask, fresh, stale[2, :, columns].astype(F32)).astype(BF16)
    for k in range(PARTS - 1):
        query_copy(k).wait_send()
        for h in range(HEADS_DEV):
            kv_copy(h, k).wait_send()
            out_copy(h, k).wait_send()


def step(
    tokens,
    projection_weight,
    shift_term,
    scale_term,
    query_gain,
    key_gain,
    stale_keys,
    stale_values,
    stale_output,
    refreshed,
):
    anywhere = pl.BlockSpec(memory_space=pl.ANY)
    vmem = pl.BlockSpec(memory_space=pltpu.VMEM)
    dma = pltpu.SemaphoreType.DMA
    others = PARTS - 1
    scratch = [
        pltpu.VMEM((ROWS, D), BF16),
        pltpu.VMEM((3, D, D), BF16),
        pltpu.VMEM((3, ROWS, D), BF16),
        pltpu.VMEM((ROWS, D), BF16),
        pltpu.VMEM((D, ROWS), BF16),
        pltpu.VMEM((ROWS, 128), F32),
        pltpu.VMEM((PARTS, HEADS_DEV, HD, ROWS), BF16),
        pltpu.VMEM((HEADS_DEV, PARTS, 2, HD, ROWS), BF16),
        pltpu.VMEM((PARTS, HEADS_DEV, HD, ROWS), BF16),
        pltpu.VMEM((HEADS_DEV, PARTS, 2, HD, ROWS), BF16),
        pltpu.VMEM((HEADS_DEV, TILES, TILE, HD), BF16),
        pltpu.VMEM((HEADS_DEV, REFRESHED, TILE, HD), BF16),
        pltpu.VMEM((HEADS_DEV, FRESH, HD), F32),
        pltpu.VMEM((HEADS_DEV, FRESH, 128), F32),
        pltpu.VMEM((HEADS_DEV, REFRESHED, TILE, HD), BF16),
        pltpu.VMEM((HEADS_DEV, PARTS, HD, ROWS), BF16),
        pltpu.VMEM((PARTS, HEADS_DEV, HD, ROWS), BF16),
        pltpu.VMEM((2, 256), jnp.int32),
        pltpu.SMEM((2, 256), jnp.int32),
        dma((TOKEN_LOADS,)),
        dma((3,)),
        dma((3,)),
        dma,
        dma((5,)),
        dma((others,)),
        dma((others,)),
        dma((HEADS_DEV, others)),
        dma((HEADS_DEV, others)),
        dma((HEADS_DEV, others)),
        dma((HEADS_DEV, others)),
    ]
    return pl.pallas_call(
        kernel,
        out_shape=jax.ShapeDtypeStruct((ROWS, D), BF16),
        in_specs=[anywhere, anywhere, vmem, vmem, vmem, vmem, anywhere, anywhere, anywhere, vmem],
        out_specs=vmem,
        scratch_shapes=scratch,
        compiler_params=pltpu.CompilerParams(
            collective_id=0, has_side_effects=True, vmem_limit_bytes=60 * 2**20
        ),
    )(
        tokens,
        projection_weight,
        shift_term,
        scale_term,
        query_gain,
        key_gain,
        stale_keys,
        stale_values,
        stale_output,
        refreshed,
    )


def solution(mesh):
    rows = P(("grp", "patch"), None)
    in_specs = (rows, P(), P(), P(), P(), P(), rows, rows, rows, P("grp"))
    return jax.shard_map(step, mesh=mesh, in_specs=in_specs, out_specs=rows, check_vma=False)
```

```python
import functools
import math

import jax
import jax.numpy as jnp
from jax import lax
from jax.experimental import pallas as pl
from jax.experimental.pallas import tpu as pltpu
from jax.sharding import PartitionSpec as P

H = 16
HD = 72
TILE = 16
D = H * HD
PARTS = 8
ROWS = 384
TILES_DEV = ROWS // TILE
TILES = PARTS * TILES_DEV
REFRESHED = 64
FRESH = REFRESHED * TILE
HEADS_DEV = H // PARTS
BLOCK = 384
QBLOCK = 256
QUERY_PARTS = 3
QUERY_ROWS = ROWS // QUERY_PARTS
NORM_BLOCK = 32
MESH = pl.DeviceIdType.MESH
EPSILON = 1e-06
F32 = jnp.float32
BF16 = jnp.bfloat16

OFFSETS = ((2, 1), (2, 0), (1, 1), (3, 1), (0, 1), (1, 0), (3, 0))


def dot(a, b):
    return jnp.dot(a, b, preferred_element_type=F32)


def dot_nt(a, b):
    return lax.dot_general(a, b, (((1,), (1,)), ((), ())), preferred_element_type=F32)


def eye(n):
    rows = lax.broadcasted_iota(jnp.int32, (n, n), 0)
    columns = lax.broadcasted_iota(jnp.int32, (n, n), 1)
    return jnp.where(rows == columns, 1.0, 0.0).astype(BF16)


def kernel(
    tokens_hbm,
    weight_hbm,
    shift_hbm,
    scale_hbm,
    query_gain_hbm,
    key_gain_hbm,
    stale_keys_hbm,
    stale_values_hbm,
    stale_output_hbm,
    refreshed_hbm,
    out_ref,
    shift_ref,
    scale_ref,
    query_gain_ref,
    key_gain_ref,
    refreshed_ref,
    tokens,
    weight,
    stale,
    hidden,
    turned,
    own_mask,
    query_send,
    kv_send,
    query_recv,
    kv_recv,
    query_rows,
    query_fresh,
    numerator,
    totals,
    attended,
    out_send,
    out_recv,
    plan_vmem,
    plan,
    small_sem,
    load_sem,
    weight_sem,
    stale_sem,
    plan_sem,
    own_sem,
    q_send_sem,
    q_recv_sem,
    kv_send_sem,
    kv_recv_sem,
    o_send_sem,
    o_recv_sem,
):
    grp = lax.axis_index("grp")
    me = lax.axis_index("patch")
    my_y, my_x = me // 2, me % 2

    def target(k):
        dy, dx = OFFSETS[k]
        return lax.rem(my_y + dy, 4) * 2 + lax.rem(my_x + dx, 2)

    def source(k):
        dy, dx = OFFSETS[k]
        return lax.rem(my_y + 4 - dy, 4) * 2 + lax.rem(my_x + dx, 2)

    barrier = pltpu.get_barrier_semaphore()
    for k in range(PARTS - 1):
        pl.semaphore_signal(barrier, inc=1, device_id=(grp, target(k)), device_id_type=MESH)

    small = (
        (shift_hbm, shift_ref),
        (scale_hbm, scale_ref),
        (query_gain_hbm, query_gain_ref),
        (key_gain_hbm, key_gain_ref),
        (refreshed_hbm, refreshed_ref),
    )
    small_loads = [
        pltpu.make_async_copy(there, here, small_sem.at[at]) for at, (there, here) in enumerate(small)
    ]
    loads = []
    for part in range(QUERY_PARTS):
        rows = pl.ds(part * (ROWS // QUERY_PARTS), ROWS // QUERY_PARTS)
        loads.append(pltpu.make_async_copy(tokens_hbm.at[rows], tokens.at[rows], load_sem.at[part]))
    weight_loads = []
    for part in range(3):
        columns = pl.ds(part * D, D)
        weight_loads.append(
            pltpu.make_async_copy(weight_hbm.at[:, columns], weight.at[part], weight_sem.at[part])
        )
    stale_loads = []
    for slot, ref in enumerate((stale_keys_hbm, stale_values_hbm, stale_output_hbm)):
        stale_loads.append(pltpu.make_async_copy(ref, stale.at[slot], stale_sem.at[slot]))
    loads[0].start()
    for load in small_loads[:3]:
        load.start()
    weight_loads[0].start()
    for load in loads[1:] + small_loads[3:]:
        load.start()
    for part in range(3):
        if part > 0:
            weight_loads[part].start()
        stale_loads[part].start()

    def column(gain_ref):
        same = lax.broadcasted_iota(jnp.int32, (HD, HD), 0) == lax.broadcasted_iota(
            jnp.int32, (HD, HD), 1
        )
        row = jnp.broadcast_to(gain_ref[...].reshape(1, HD), (HD, HD))
        return jnp.sum(jnp.where(same, row, 0.0), axis=1, keepdims=True)

    for load in small_loads[:3]:
        load.wait()
    shift = shift_ref[...].reshape(1, D)
    scale = 1.0 + scale_ref[...].reshape(1, D)

    def modulate(first, count):
        for block in range(count // NORM_BLOCK):
            rows = pl.ds(first + block * NORM_BLOCK, NORM_BLOCK)
            values = tokens[rows, :].astype(F32)
            center = values - jnp.mean(values, axis=-1, keepdims=True)
            spread = jnp.mean(center * center, axis=-1, keepdims=True)
            normed = center * (1.0 / jnp.sqrt(spread + EPSILON))
            hidden[rows, :] = (normed * scale + shift).astype(BF16)

    def project(part):
        for block in range(D // BLOCK):
            columns = pl.ds(block * BLOCK, BLOCK)
            fresh = dot(hidden[...], weight[part, :, columns]).astype(BF16)
            mask = own_mask[...]
            mask = jnp.concatenate([mask] * (BLOCK // 128), axis=1)
            old = stale[part - 1, :, columns].astype(F32)
            fresh = jnp.where(mask > 0.5, fresh.astype(F32), old).astype(BF16)
            turned[columns, :] = fresh.T

    def head_norm(values, gain):
        values = values.astype(F32)
        mean = jnp.sum(values * values, axis=0, keepdims=True) * (1.0 / HD)
        return (values * (1.0 / jnp.sqrt(mean + EPSILON)) * gain).astype(BF16)

    def query_copy(part, k):
        return pltpu.make_async_remote_copy(
            src_ref=query_send.at[part, target(k)],
            dst_ref=query_recv.at[part, me],
            send_sem=q_send_sem.at[part, k],
            recv_sem=q_recv_sem.at[part, k],
            device_id=(grp, target(k)),
            device_id_type=MESH,
        )

    def kv_copy(head, k):
        return pltpu.make_async_remote_copy(
            src_ref=kv_send.at[head, target(k)],
            dst_ref=kv_recv.at[head, me],
            send_sem=kv_send_sem.at[head, k],
            recv_sem=kv_recv_sem.at[head, k],
            device_id=(grp, target(k)),
            device_id_type=MESH,
        )

    def out_copy(head, k):
        return pltpu.make_async_remote_copy(
            src_ref=out_send.at[head, target(k)],
            dst_ref=out_recv.at[me, head],
            send_sem=o_send_sem.at[head, k],
            recv_sem=o_recv_sem.at[head, k],
            device_id=(grp, target(k)),
            device_id_type=MESH,
        )

    own_out = [
        pltpu.make_async_copy(out_send.at[h, me], out_recv.at[me, h], own_sem.at[h])
        for h in range(HEADS_DEV)
    ]

    gain = column(query_gain_ref)
    for part in range(QUERY_PARTS):
        with jax.named_scope("norm"):
            loads[part].wait()
            modulate(part * QUERY_ROWS, QUERY_ROWS)
        with jax.named_scope("proj_q"):
            if part == 0:
                weight_loads[0].wait()
            rows = pl.ds(part * QUERY_ROWS, QUERY_ROWS)
            for block in range(D // BLOCK):
                columns = pl.ds(block * BLOCK, BLOCK)
                fresh = dot(hidden[rows, :], weight[0, :, columns]).astype(BF16)
                turned[columns, rows] = fresh.T
        with jax.named_scope("norm_q"):
            for head in range(H):
                query_send[part, head // HEADS_DEV, head % HEADS_DEV] = head_norm(
                    turned[pl.ds(head * HD, HD), rows], gain
                )
        if part == 0:
            with jax.named_scope("barrier"):
                pl.semaphore_wait(barrier, PARTS - 1)
        for k in range(PARTS - 1):
            query_copy(part, k).start()

    for load in small_loads[3:]:
        load.wait()
    flags = refreshed_ref[...].reshape(1, TILES).astype(F32)
    tile_row = lax.broadcasted_iota(jnp.int32, (TILES, TILES), 0)
    tile_col = lax.broadcasted_iota(jnp.int32, (TILES, TILES), 1)
    flag_rows = jnp.broadcast_to(flags, (TILES, TILES))
    until = jnp.where(tile_col <= tile_row, flag_rows, 0.0).astype(BF16)
    inclusive = dot(until, jnp.ones((TILES, 128), BF16))
    slots = lax.broadcasted_iota(jnp.int32, (TILES, 128), 1).astype(F32)
    which = jnp.sum(jnp.where(inclusive <= slots, 1.0, 0.0), axis=0, keepdims=True)
    which = jnp.minimum(which, float(TILES - 1))
    before = jnp.where(tile_row < tile_col, 1.0, 0.0).astype(BF16)
    rank = dot(jnp.broadcast_to(flags, (8, TILES)).astype(BF16), before)[0:1]
    rank = jnp.minimum(rank, float(REFRESHED - 1))
    plan_vmem[0:1, 0:128] = which.astype(jnp.int32)
    plan_vmem[1:2, 0:TILES] = rank.astype(jnp.int32)
    plan_copy = pltpu.make_async_copy(plan_vmem, plan, plan_sem)
    plan_copy.start()
    row_tile = lax.broadcasted_iota(jnp.int32, (ROWS, TILES), 0) // TILE + me * TILES_DEV
    row_col = lax.broadcasted_iota(jnp.int32, (ROWS, TILES), 1)
    chosen = jnp.where(row_tile == row_col, jnp.broadcast_to(flags, (ROWS, TILES)), 0.0)
    own_mask[...] = dot(chosen.astype(BF16), jnp.ones((TILES, 128), BF16))

    with jax.named_scope("proj_k"):
        weight_loads[1].wait()
        stale_loads[0].wait()
        project(1)
    with jax.named_scope("norm_k"):
        gain = column(key_gain_ref)
        for head in range(H):
            values = turned[pl.ds(head * HD, HD), :]
            kv_send[head % HEADS_DEV, head // HEADS_DEV, 0] = head_norm(values, gain)
    with jax.named_scope("proj_v"):
        weight_loads[2].wait()
        stale_loads[1].wait()
        project(2)
    with jax.named_scope("put_v"):
        for head in range(H):
            kv_send[head % HEADS_DEV, head // HEADS_DEV, 1] = turned[pl.ds(head * HD, HD), :]
    for h in range(HEADS_DEV):
        for k in range(PARTS - 1):
            kv_copy(h, k).start()

    numerator[...] = jnp.zeros_like(numerator)
    totals[...] = jnp.zeros_like(totals)
    same = eye(QUERY_ROWS)
    part_tiles = QUERY_ROWS // TILE

    def turn_queries(buffer, part, index):
        for h in range(HEADS_DEV):
            rows = dot_nt(same, buffer[part, index, h]).astype(BF16)
            tiles = pl.ds(index * TILES_DEV + part * part_tiles, part_tiles)
            query_rows[h, tiles] = rows.reshape(part_tiles, TILE, HD)

    with jax.named_scope("turn_q"):
        for part in range(QUERY_PARTS):
            turn_queries(query_send, part, me)
        for part in range(QUERY_PARTS):
            for k in range(PARTS - 1):
                with jax.named_scope(f"wait_q#p={part}#k={k}"):
                    query_copy(part, k).wait_recv()
                turn_queries(query_recv, part, source(k))
    with jax.named_scope("keep_fresh"):
        plan_copy.wait()
        for slot in range(REFRESHED):
            tile = jnp.clip(plan[0, slot], 0, TILES - 1)
            for h in range(HEADS_DEV):
                query_fresh[h, slot] = query_rows[h, tile]
    factor = math.log2(math.e) / math.sqrt(HD)
    tiles_block = QBLOCK // TILE

    def add_blocks(head, blocks):
        keys = jnp.concatenate([ref[head, index, 0] for ref, index in blocks], axis=1)
        values = jnp.concatenate([ref[head, index, 1] for ref, index in blocks], axis=1)
        for block in range(FRESH // QBLOCK):
            rows = pl.ds(block * QBLOCK, QBLOCK)
            queries = query_fresh[head, pl.ds(block * tiles_block, tiles_block)]
            scores = dot(queries.reshape(QBLOCK, HD), keys)
            weights = jnp.exp2(scores * factor)
            sums = weights[:, 0:128]
            for lane in range(128, ROWS * len(blocks), 128):
                sums = sums + weights[:, lane : lane + 128]
            totals[head, rows, :] += sums
            numerator[head, rows, :] += dot_nt(weights.astype(BF16), values)

    def send_out(head):
        for block in range(FRESH // QBLOCK):
            rows = pl.ds(block * QBLOCK, QBLOCK)
            total = jnp.sum(totals[head, rows, :], axis=1, keepdims=True)
            result = (numerator[head, rows, :] / total).astype(BF16)
            attended[head, pl.ds(block * tiles_block, tiles_block)] = result.reshape(
                tiles_block, TILE, HD
            )

        same = eye(HD)
        for owner in range(PARTS):
            pieces = []
            for tile in range(TILES_DEV):
                item = jnp.clip(plan[1, owner * TILES_DEV + tile], 0, REFRESHED - 1)
                pieces.append(attended[head, item])
            rows = jnp.concatenate(pieces, axis=0)
            out_send[head, owner] = dot_nt(same, rows).astype(BF16)
        for k in range(PARTS - 1):
            out_copy(head, k).start()
        own_out[head].start()

    for h in range(HEADS_DEV):
        for step in ((0,), (1, 2), (3, 4), (5, 6)):
            with jax.named_scope(f"wait_kv#h={h}#k={step[0]}"):
                for k in step:
                    kv_copy(h, k).wait_recv()
            with jax.named_scope("add"):
                blocks = [(kv_recv, source(k)) for k in step]
                if len(step) == 1:
                    blocks.append((kv_send, me))
                add_blocks(h, blocks)
        with jax.named_scope("send_out"):
            send_out(h)

    with jax.named_scope("wait_out"):
        stale_loads[2].wait()
        for h in range(HEADS_DEV):
            own_out[h].wait()
            for k in range(PARTS - 1):
                out_copy(h, k).wait_recv()
    with jax.named_scope("merge"):
        for owner in range(PARTS):
            for h in range(HEADS_DEV):
                turned[pl.ds((owner * HEADS_DEV + h) * HD, HD), :] = out_recv[owner, h]
        mask = own_mask[...] > 0.5
        for block in range(D // 128):
            columns = pl.ds(block * 128, 128)
            fresh = turned[columns, :].T.astype(F32)
            out_ref[:, columns] = jnp.where(mask, fresh, stale[2, :, columns].astype(F32)).astype(BF16)
    for k in range(PARTS - 1):
        for part in range(QUERY_PARTS):
            query_copy(part, k).wait_send()
        for h in range(HEADS_DEV):
            kv_copy(h, k).wait_send()
            out_copy(h, k).wait_send()


def step(
    tokens,
    projection_weight,
    shift_term,
    scale_term,
    query_gain,
    key_gain,
    stale_keys,
    stale_values,
    stale_output,
    refreshed,
):
    hbm = pl.BlockSpec(memory_space=pltpu.HBM)
    vmem = pl.BlockSpec(memory_space=pltpu.VMEM)
    dma = pltpu.SemaphoreType.DMA
    others = PARTS - 1
    scratch = [
        pltpu.VMEM((D,), F32),
        pltpu.VMEM((D,), F32),
        pltpu.VMEM((HD,), F32),
        pltpu.VMEM((HD,), F32),
        pltpu.VMEM((TILES,), jnp.int32),
        pltpu.VMEM((ROWS, D), BF16),
        pltpu.VMEM((3, D, D), BF16),
        pltpu.VMEM((3, ROWS, D), BF16),
        pltpu.VMEM((ROWS, D), BF16),
        pltpu.VMEM((D, ROWS), BF16),
        pltpu.VMEM((ROWS, 128), F32),
        pltpu.VMEM((QUERY_PARTS, PARTS, HEADS_DEV, HD, QUERY_ROWS), BF16),
        pltpu.VMEM((HEADS_DEV, PARTS, 2, HD, ROWS), BF16),
        pltpu.VMEM((QUERY_PARTS, PARTS, HEADS_DEV, HD, QUERY_ROWS), BF16),
        pltpu.VMEM((HEADS_DEV, PARTS, 2, HD, ROWS), BF16),
        pltpu.VMEM((HEADS_DEV, TILES, TILE, HD), BF16),
        pltpu.VMEM((HEADS_DEV, REFRESHED, TILE, HD), BF16),
        pltpu.VMEM((HEADS_DEV, FRESH, HD), F32),
        pltpu.VMEM((HEADS_DEV, FRESH, 128), F32),
        pltpu.VMEM((HEADS_DEV, REFRESHED, TILE, HD), BF16),
        pltpu.VMEM((HEADS_DEV, PARTS, HD, ROWS), BF16),
        pltpu.VMEM((PARTS, HEADS_DEV, HD, ROWS), BF16),
        pltpu.VMEM((2, 256), jnp.int32),
        pltpu.SMEM((2, 256), jnp.int32),
        dma((5,)),
        dma((QUERY_PARTS,)),
        dma((3,)),
        dma((3,)),
        dma,
        dma((HEADS_DEV,)),
        dma((QUERY_PARTS, others)),
        dma((QUERY_PARTS, others)),
        dma((HEADS_DEV, others)),
        dma((HEADS_DEV, others)),
        dma((HEADS_DEV, others)),
        dma((HEADS_DEV, others)),
    ]
    return pl.pallas_call(
        kernel,
        out_shape=jax.ShapeDtypeStruct((ROWS, D), BF16),
        in_specs=[hbm] * 10,
        out_specs=vmem,
        scratch_shapes=scratch,
        compiler_params=pltpu.CompilerParams(
            collective_id=0, has_side_effects=True, vmem_limit_bytes=63 * 2**20
        ),
    )(
        tokens,
        projection_weight,
        shift_term,
        scale_term,
        query_gain,
        key_gain,
        stale_keys,
        stale_values,
        stale_output,
        refreshed,
    )


def solution(mesh):
    rows = P(("grp", "patch"), None)
    in_specs = (rows, P(), P(), P(), P(), P(), rows, rows, rows, P("grp"))
    return jax.shard_map(step, mesh=mesh, in_specs=in_specs, out_specs=rows, check_vma=False)
```

```python
import functools
import math

import jax
import jax.numpy as jnp
from jax import lax
from jax.experimental import pallas as pl
from jax.experimental.pallas import tpu as pltpu
from jax.sharding import PartitionSpec as P

H = 16
HD = 72
TILE = 16
D = H * HD
PARTS = 8
ROWS = 384
TILES_DEV = ROWS // TILE
TILES = PARTS * TILES_DEV
REFRESHED = 64
FRESH = REFRESHED * TILE
HEADS_DEV = H // PARTS
BLOCK = 384
QBLOCK = 256
QUERY_PARTS = 3
STEPS = (
    (0, (0,)),
    (0, (1, 2)),
    (0, (3, 4)),
    (1, (0,)),
    (0, (5, 6)),
    (1, (1, 2)),
    (1, (3, 4)),
    (1, (5, 6)),
)
QUERY_ROWS = ROWS // QUERY_PARTS
NORM_BLOCK = 32
MESH = pl.DeviceIdType.MESH
EPSILON = 1e-06
F32 = jnp.float32
BF16 = jnp.bfloat16

OFFSETS = ((2, 1), (2, 0), (1, 1), (3, 1), (0, 1), (1, 0), (3, 0))

STEP_OF = (0, 1, 1, 2, 2, 3, 3)


def dot(a, b):
    return jnp.dot(a, b, preferred_element_type=F32)


def dot_nt(a, b):
    return lax.dot_general(a, b, (((1,), (1,)), ((), ())), preferred_element_type=F32)


def eye(n):
    rows = lax.broadcasted_iota(jnp.int32, (n, n), 0)
    columns = lax.broadcasted_iota(jnp.int32, (n, n), 1)
    return jnp.where(rows == columns, 1.0, 0.0).astype(BF16)


def kernel(
    tokens_hbm,
    weight_hbm,
    shift_hbm,
    scale_hbm,
    query_gain_hbm,
    key_gain_hbm,
    stale_keys_hbm,
    stale_values_hbm,
    stale_output_hbm,
    refreshed_hbm,
    out_hbm,
    shift_ref,
    scale_ref,
    query_gain_ref,
    key_gain_ref,
    refreshed_ref,
    tokens,
    weight,
    stale,
    hidden,
    turned,
    own_mask,
    query_send,
    kv_send,
    query_recv,
    kv_recv,
    query_rows,
    query_fresh,
    numerator,
    totals,
    attended,
    out_send,
    out_recv,
    result,
    plan_vmem,
    plan,
    small_sem,
    load_sem,
    weight_sem,
    stale_sem,
    plan_sem,
    store_sem,
    own_sem,
    q_send_sem,
    q_recv_sem,
    kv_send_sem,
    kv_recv_sem,
    o_send_sem,
    o_recv_sem,
):
    grp = lax.axis_index("grp")
    me = lax.axis_index("patch")
    my_y, my_x = me // 2, me % 2

    def target(k):
        dy, dx = OFFSETS[k]
        return lax.rem(my_y + dy, 4) * 2 + lax.rem(my_x + dx, 2)

    def source(k):
        dy, dx = OFFSETS[k]
        return lax.rem(my_y + 4 - dy, 4) * 2 + lax.rem(my_x + dx, 2)

    barrier = pltpu.get_barrier_semaphore()
    for k in range(PARTS - 1):
        pl.semaphore_signal(barrier, inc=1, device_id=(grp, target(k)), device_id_type=MESH)

    small = (
        (shift_hbm, shift_ref),
        (scale_hbm, scale_ref),
        (query_gain_hbm, query_gain_ref),
        (key_gain_hbm, key_gain_ref),
        (refreshed_hbm, refreshed_ref),
    )
    small_loads = [
        pltpu.make_async_copy(there, here, small_sem.at[at]) for at, (there, here) in enumerate(small)
    ]
    loads = []
    for part in range(QUERY_PARTS):
        rows = pl.ds(part * (ROWS // QUERY_PARTS), ROWS // QUERY_PARTS)
        loads.append(pltpu.make_async_copy(tokens_hbm.at[rows], tokens.at[rows], load_sem.at[part]))
    weight_loads = []
    for part in range(3):
        columns = pl.ds(part * D, D)
        weight_loads.append(
            pltpu.make_async_copy(weight_hbm.at[:, columns], weight.at[part], weight_sem.at[part])
        )
    stale_loads = []
    for slot, ref in enumerate((stale_keys_hbm, stale_values_hbm, stale_output_hbm)):
        stale_loads.append(pltpu.make_async_copy(ref, stale.at[slot], stale_sem.at[slot]))
    loads[0].start()
    for load in small_loads[:3]:
        load.start()
    weight_loads[0].start()
    for load in loads[1:] + small_loads[3:]:
        load.start()
    for part in range(3):
        if part > 0:
            weight_loads[part].start()
        stale_loads[part].start()

    def column(gain_ref):
        same = lax.broadcasted_iota(jnp.int32, (HD, HD), 0) == lax.broadcasted_iota(
            jnp.int32, (HD, HD), 1
        )
        row = jnp.broadcast_to(gain_ref[...].reshape(1, HD), (HD, HD))
        return jnp.sum(jnp.where(same, row, 0.0), axis=1, keepdims=True)

    for load in small_loads[:3]:
        load.wait()
    shift = shift_ref[...].reshape(1, D)
    scale = 1.0 + scale_ref[...].reshape(1, D)

    def modulate(first, count):
        for block in range(count // NORM_BLOCK):
            rows = pl.ds(first + block * NORM_BLOCK, NORM_BLOCK)
            values = tokens[rows, :].astype(F32)
            center = values - jnp.mean(values, axis=-1, keepdims=True)
            spread = jnp.mean(center * center, axis=-1, keepdims=True)
            normed = center * (1.0 / jnp.sqrt(spread + EPSILON))
            hidden[rows, :] = (normed * scale + shift).astype(BF16)

    def project(part):
        for block in range(D // BLOCK):
            columns = pl.ds(block * BLOCK, BLOCK)
            fresh = dot(hidden[...], weight[part, :, columns]).astype(BF16)
            mask = own_mask[...]
            mask = jnp.concatenate([mask] * (BLOCK // 128), axis=1)
            old = stale[part - 1, :, columns].astype(F32)
            fresh = jnp.where(mask > 0.5, fresh.astype(F32), old).astype(BF16)
            turned[columns, :] = fresh.T

    def head_norm(values, gain):
        values = values.astype(F32)
        mean = jnp.sum(values * values, axis=0, keepdims=True) * (1.0 / HD)
        return (values * (1.0 / jnp.sqrt(mean + EPSILON)) * gain).astype(BF16)

    def query_copy(part, k):
        return pltpu.make_async_remote_copy(
            src_ref=query_send.at[part, target(k)],
            dst_ref=query_recv.at[part, me],
            send_sem=q_send_sem,
            recv_sem=q_recv_sem.at[k],
            device_id=(grp, target(k)),
            device_id_type=MESH,
        )

    def kv_copy(head, k):
        return pltpu.make_async_remote_copy(
            src_ref=kv_send.at[head, target(k)],
            dst_ref=kv_recv.at[head, me],
            send_sem=kv_send_sem,
            recv_sem=kv_recv_sem.at[head, STEP_OF[k]],
            device_id=(grp, target(k)),
            device_id_type=MESH,
        )

    def out_copy(head, k):
        return pltpu.make_async_remote_copy(
            src_ref=out_send.at[head, target(k)],
            dst_ref=out_recv.at[me, head],
            send_sem=o_send_sem,
            recv_sem=o_recv_sem,
            device_id=(grp, target(k)),
            device_id_type=MESH,
        )

    def own_out(head):
        return pltpu.make_async_copy(out_send.at[head, me], out_recv.at[me, head], own_sem)

    def wait_bytes(ref, sem):
        pltpu.make_async_copy(ref, ref, sem).wait()

    gain = column(query_gain_ref)
    for part in range(QUERY_PARTS):
        with jax.named_scope("norm"):
            loads[part].wait()
            modulate(part * QUERY_ROWS, QUERY_ROWS)
        with jax.named_scope("proj_q"):
            if part == 0:
                weight_loads[0].wait()
            rows = pl.ds(part * QUERY_ROWS, QUERY_ROWS)
            for block in range(D // BLOCK):
                columns = pl.ds(block * BLOCK, BLOCK)
                fresh = dot(hidden[rows, :], weight[0, :, columns]).astype(BF16)
                turned[columns, rows] = fresh.T
        with jax.named_scope("norm_q"):
            for head in range(H):
                query_send[part, head // HEADS_DEV, head % HEADS_DEV] = head_norm(
                    turned[pl.ds(head * HD, HD), rows], gain
                )
        if part == 0:
            with jax.named_scope("barrier"):
                pl.semaphore_wait(barrier, PARTS - 1)
        for k in range(PARTS - 1):
            query_copy(part, k).start()

    for load in small_loads[3:]:
        load.wait()
    flags = refreshed_ref[...].reshape(1, TILES).astype(F32)
    tile_row = lax.broadcasted_iota(jnp.int32, (TILES, TILES), 0)
    tile_col = lax.broadcasted_iota(jnp.int32, (TILES, TILES), 1)
    flag_rows = jnp.broadcast_to(flags, (TILES, TILES))
    until = jnp.where(tile_col <= tile_row, flag_rows, 0.0).astype(BF16)
    inclusive = dot(until, jnp.ones((TILES, 128), BF16))
    slots = lax.broadcasted_iota(jnp.int32, (TILES, 128), 1).astype(F32)
    which = jnp.sum(jnp.where(inclusive <= slots, 1.0, 0.0), axis=0, keepdims=True)
    which = jnp.minimum(which, float(TILES - 1))
    before = jnp.where(tile_row < tile_col, 1.0, 0.0).astype(BF16)
    rank = dot(jnp.broadcast_to(flags, (8, TILES)).astype(BF16), before)[0:1]
    rank = jnp.minimum(rank, float(REFRESHED - 1))
    plan_vmem[0:1, 0:128] = which.astype(jnp.int32)
    plan_vmem[1:2, 0:TILES] = rank.astype(jnp.int32)
    plan_copy = pltpu.make_async_copy(plan_vmem, plan, plan_sem)
    plan_copy.start()
    row_tile = lax.broadcasted_iota(jnp.int32, (ROWS, TILES), 0) // TILE + me * TILES_DEV
    row_col = lax.broadcasted_iota(jnp.int32, (ROWS, TILES), 1)
    chosen = jnp.where(row_tile == row_col, jnp.broadcast_to(flags, (ROWS, TILES)), 0.0)
    own_mask[...] = dot(chosen.astype(BF16), jnp.ones((TILES, 128), BF16))

    with jax.named_scope("proj_k"):
        weight_loads[1].wait()
        stale_loads[0].wait()
        project(1)
    with jax.named_scope("norm_k"):
        gain = column(key_gain_ref)
        for head in range(H):
            values = turned[pl.ds(head * HD, HD), :]
            kv_send[head % HEADS_DEV, head // HEADS_DEV, 0] = head_norm(values, gain)
    with jax.named_scope("proj_v"):
        weight_loads[2].wait()
        stale_loads[1].wait()
        project(2)
    with jax.named_scope("put_v"):
        for head in range(H):
            kv_send[head % HEADS_DEV, head // HEADS_DEV, 1] = turned[pl.ds(head * HD, HD), :]
    for h in range(HEADS_DEV):
        for k in range(PARTS - 1):
            kv_copy(h, k).start()

    numerator[...] = jnp.zeros_like(numerator)
    totals[...] = jnp.zeros_like(totals)
    same = eye(QUERY_ROWS)
    part_tiles = QUERY_ROWS // TILE

    def turn_queries(buffer, part, index):
        for h in range(HEADS_DEV):
            rows = dot_nt(same, buffer[part, index, h]).astype(BF16)
            tiles = pl.ds(index * TILES_DEV + part * part_tiles, part_tiles)
            query_rows[h, tiles] = rows.reshape(part_tiles, TILE, HD)

    with jax.named_scope("turn_q"):
        for part in range(QUERY_PARTS):
            turn_queries(query_send, part, me)
        for k in range(PARTS - 1):
            with jax.named_scope(f"wait_q#k={k}"):
                wait_bytes(query_recv.at[:, source(k)], q_recv_sem.at[k])
            for part in range(QUERY_PARTS):
                turn_queries(query_recv, part, source(k))
    with jax.named_scope("keep_fresh"):
        plan_copy.wait()
        for slot in range(REFRESHED):
            tile = jnp.clip(plan[0, slot], 0, TILES - 1)
            for h in range(HEADS_DEV):
                query_fresh[h, slot] = query_rows[h, tile]
    factor = math.log2(math.e) / math.sqrt(HD)
    tiles_block = QBLOCK // TILE

    def add_blocks(head, blocks):
        keys = jnp.concatenate([ref[head, index, 0] for ref, index in blocks], axis=1)
        values = jnp.concatenate([ref[head, index, 1] for ref, index in blocks], axis=1)
        for block in range(FRESH // QBLOCK):
            rows = pl.ds(block * QBLOCK, QBLOCK)
            queries = query_fresh[head, pl.ds(block * tiles_block, tiles_block)]
            scores = dot(queries.reshape(QBLOCK, HD), keys)
            weights = jnp.exp2(scores * factor)
            sums = weights[:, 0:128]
            for lane in range(128, ROWS * len(blocks), 128):
                sums = sums + weights[:, lane : lane + 128]
            totals[head, rows, :] += sums
            numerator[head, rows, :] += dot_nt(weights.astype(BF16), values)

    def send_out(head):
        for block in range(FRESH // QBLOCK):
            rows = pl.ds(block * QBLOCK, QBLOCK)
            total = jnp.sum(totals[head, rows, :], axis=1, keepdims=True)
            result = (numerator[head, rows, :] / total).astype(BF16)
            attended[head, pl.ds(block * tiles_block, tiles_block)] = result.reshape(
                tiles_block, TILE, HD
            )

        same = eye(HD)
        for owner in range(PARTS):
            pieces = []
            for tile in range(TILES_DEV):
                item = jnp.clip(plan[1, owner * TILES_DEV + tile], 0, REFRESHED - 1)
                pieces.append(attended[head, item])
            rows = jnp.concatenate(pieces, axis=0)
            out_send[head, owner] = dot_nt(same, rows).astype(BF16)
        for k in range(PARTS - 1):
            out_copy(head, k).start()
        own_out(head).start()

    for h, step in STEPS:
        with jax.named_scope(f"wait_kv#h={h}#k={step[0]}"):
            wait_bytes(kv_recv.at[h, pl.ds(0, len(step))], kv_recv_sem.at[h, STEP_OF[step[0]]])
        with jax.named_scope("add"):
            blocks = [(kv_recv, source(k)) for k in step]
            if len(step) == 1:
                blocks.append((kv_send, me))
            add_blocks(h, blocks)
        if step == STEPS[-1][1]:
            with jax.named_scope("send_out"):
                send_out(h)

    with jax.named_scope("wait_out"):
        stale_loads[2].wait()
        wait_bytes(out_recv.at[me], own_sem)
        wait_bytes(out_recv.at[pl.ds(0, PARTS - 1)], o_recv_sem)
    with jax.named_scope("merge"):
        mask = own_mask[...] > 0.5
        for block in range(D // 128):
            columns = pl.ds(block * 128, 128)
            heads = range(block * 128 // HD, (block * 128 + 127) // HD + 1)
            for head in heads:
                if head * HD >= block * 128 or block == 0:
                    turned[pl.ds(head * HD, HD), :] = out_recv[head // HEADS_DEV, head % HEADS_DEV]
            fresh = turned[columns, :].T.astype(F32)
            old = stale[2, :, columns].astype(F32)
            result[:, columns] = jnp.where(mask, fresh, old).astype(BF16)
            if block % 3 == 2:
                columns = pl.ds((block - 2) * 128, 3 * 128)
                pltpu.make_async_copy(
                    result.at[:, columns], out_hbm.at[:, columns], store_sem
                ).start()
    with jax.named_scope("wait_end"):
        wait_bytes(query_send.at[:, pl.ds(0, PARTS - 1)], q_send_sem)
        wait_bytes(kv_send.at[:, pl.ds(0, PARTS - 1)], kv_send_sem)
        wait_bytes(out_send.at[:, pl.ds(0, PARTS - 1)], o_send_sem)
        pltpu.make_async_copy(result, out_hbm, store_sem).wait()


def step(
    tokens,
    projection_weight,
    shift_term,
    scale_term,
    query_gain,
    key_gain,
    stale_keys,
    stale_values,
    stale_output,
    refreshed,
):
    hbm = pl.BlockSpec(memory_space=pltpu.HBM)
    dma = pltpu.SemaphoreType.DMA
    others = PARTS - 1
    scratch = [
        pltpu.VMEM((D,), F32),
        pltpu.VMEM((D,), F32),
        pltpu.VMEM((HD,), F32),
        pltpu.VMEM((HD,), F32),
        pltpu.VMEM((TILES,), jnp.int32),
        pltpu.VMEM((ROWS, D), BF16),
        pltpu.VMEM((3, D, D), BF16),
        pltpu.VMEM((3, ROWS, D), BF16),
        pltpu.VMEM((ROWS, D), BF16),
        pltpu.VMEM((D, ROWS), BF16),
        pltpu.VMEM((ROWS, 128), F32),
        pltpu.VMEM((QUERY_PARTS, PARTS, HEADS_DEV, HD, QUERY_ROWS), BF16),
        pltpu.VMEM((HEADS_DEV, PARTS, 2, HD, ROWS), BF16),
        pltpu.VMEM((QUERY_PARTS, PARTS, HEADS_DEV, HD, QUERY_ROWS), BF16),
        pltpu.VMEM((HEADS_DEV, PARTS, 2, HD, ROWS), BF16),
        pltpu.VMEM((HEADS_DEV, TILES, TILE, HD), BF16),
        pltpu.VMEM((HEADS_DEV, REFRESHED, TILE, HD), BF16),
        pltpu.VMEM((HEADS_DEV, FRESH, HD), F32),
        pltpu.VMEM((HEADS_DEV, FRESH, 128), F32),
        pltpu.VMEM((HEADS_DEV, REFRESHED, TILE, HD), BF16),
        pltpu.VMEM((HEADS_DEV, PARTS, HD, ROWS), BF16),
        pltpu.VMEM((PARTS, HEADS_DEV, HD, ROWS), BF16),
        pltpu.VMEM((ROWS, D), BF16),
        pltpu.VMEM((2, 256), jnp.int32),
        pltpu.SMEM((2, 256), jnp.int32),
        dma((5,)),
        dma((QUERY_PARTS,)),
        dma((3,)),
        dma((3,)),
        dma,
        dma,
        dma,
        dma,
        dma((others,)),
        dma,
        dma((HEADS_DEV, 4)),
        dma,
        dma,
    ]
    return pl.pallas_call(
        kernel,
        out_shape=jax.ShapeDtypeStruct((ROWS, D), BF16),
        in_specs=[hbm] * 10,
        out_specs=hbm,
        scratch_shapes=scratch,
        compiler_params=pltpu.CompilerParams(
            collective_id=0, has_side_effects=True, vmem_limit_bytes=63 * 2**20
        ),
    )(
        tokens,
        projection_weight,
        shift_term,
        scale_term,
        query_gain,
        key_gain,
        stale_keys,
        stale_values,
        stale_output,
        refreshed,
    )


def solution(mesh):
    rows = P(("grp", "patch"), None)
    in_specs = (rows, P(), P(), P(), P(), P(), rows, rows, rows, P("grp"))
    return jax.shard_map(step, mesh=mesh, in_specs=in_specs, out_specs=rows, check_vma=False)
```

```python
import functools
import math

import jax
import jax.numpy as jnp
from jax import lax
from jax.experimental import pallas as pl
from jax.experimental.pallas import tpu as pltpu
from jax.sharding import PartitionSpec as P

H = 16
HD = 72
TILE = 16
D = H * HD
PARTS = 8
ROWS = 384
TILES_DEV = ROWS // TILE
TILES = PARTS * TILES_DEV
REFRESHED = 64
FRESH = REFRESHED * TILE
HEADS_DEV = H // PARTS
BLOCK = 384
QBLOCK = 256
QUERY_PARTS = 3
STEPS = (
    (0, (0,)),
    (0, (1, 2)),
    (0, (3, 4)),
    (1, (0,)),
    (0, (5, 6)),
    (1, (1, 2)),
    (1, (3, 4)),
    (1, (5, 6)),
)
QUERY_ROWS = ROWS // QUERY_PARTS
NORM_BLOCK = 32
MESH = pl.DeviceIdType.MESH
EPSILON = 1e-06
F32 = jnp.float32
BF16 = jnp.bfloat16

OFFSETS = ((2, 1), (2, 0), (1, 1), (3, 1), (0, 1), (1, 0), (3, 0))

STEP_OF = (0, 1, 1, 2, 2, 3, 3)


def dot(a, b):
    return jnp.dot(a, b, preferred_element_type=F32)


def dot_nt(a, b):
    return lax.dot_general(a, b, (((1,), (1,)), ((), ())), preferred_element_type=F32)


def eye(n):
    rows = lax.broadcasted_iota(jnp.int32, (n, n), 0)
    columns = lax.broadcasted_iota(jnp.int32, (n, n), 1)
    return jnp.where(rows == columns, 1.0, 0.0).astype(BF16)


def kernel(
    tokens_hbm,
    weight_hbm,
    shift_hbm,
    scale_hbm,
    query_gain_hbm,
    key_gain_hbm,
    stale_keys_hbm,
    stale_values_hbm,
    stale_output_hbm,
    refreshed_hbm,
    out_hbm,
    shift_ref,
    scale_ref,
    query_gain_ref,
    key_gain_ref,
    refreshed_ref,
    tokens,
    weight,
    stale,
    hidden,
    turned,
    own_mask,
    query_send,
    kv_send,
    query_recv,
    kv_recv,
    query_rows,
    query_fresh,
    numerator,
    totals,
    attended,
    out_send,
    out_recv,
    result,
    plan_vmem,
    plan,
    small_sem,
    load_sem,
    weight_sem,
    stale_sem,
    plan_sem,
    store_sem,
    own_sem,
    q_send_sem,
    q_recv_sem,
    kv_send_sem,
    kv_recv_sem,
    o_send_sem,
    o_recv_sem,
):
    grp = lax.axis_index("grp")
    me = lax.axis_index("patch")
    my_y, my_x = me // 2, me % 2

    def target(k):
        dy, dx = OFFSETS[k]
        return lax.rem(my_y + dy, 4) * 2 + lax.rem(my_x + dx, 2)

    def source(k):
        dy, dx = OFFSETS[k]
        return lax.rem(my_y + 4 - dy, 4) * 2 + lax.rem(my_x + dx, 2)

    barrier = pltpu.get_barrier_semaphore()
    for k in range(PARTS - 1):
        pl.semaphore_signal(barrier, inc=1, device_id=(grp, target(k)), device_id_type=MESH)

    small = (
        (shift_hbm, shift_ref),
        (scale_hbm, scale_ref),
        (query_gain_hbm, query_gain_ref),
        (key_gain_hbm, key_gain_ref),
        (refreshed_hbm, refreshed_ref),
    )
    small_loads = [
        pltpu.make_async_copy(there, here, small_sem.at[at]) for at, (there, here) in enumerate(small)
    ]
    loads = []
    for part in range(QUERY_PARTS):
        rows = pl.ds(part * (ROWS // QUERY_PARTS), ROWS // QUERY_PARTS)
        loads.append(pltpu.make_async_copy(tokens_hbm.at[rows], tokens.at[rows], load_sem.at[part]))
    weight_loads = []
    for part in range(3):
        columns = pl.ds(part * D, D)
        weight_loads.append(
            pltpu.make_async_copy(weight_hbm.at[:, columns], weight.at[part], weight_sem.at[part])
        )
    stale_loads = []
    for slot, ref in enumerate((stale_keys_hbm, stale_values_hbm, stale_output_hbm)):
        stale_loads.append(pltpu.make_async_copy(ref, stale.at[slot], stale_sem.at[slot]))
    loads[0].start()
    for load in small_loads[:3]:
        load.start()
    weight_loads[0].start()
    for load in loads[1:] + small_loads[3:]:
        load.start()
    for part in range(3):
        if part > 0:
            weight_loads[part].start()
        stale_loads[part].start()

    def column(gain_ref):
        same = lax.broadcasted_iota(jnp.int32, (HD, HD), 0) == lax.broadcasted_iota(
            jnp.int32, (HD, HD), 1
        )
        row = jnp.broadcast_to(gain_ref[...].reshape(1, HD), (HD, HD))
        return jnp.sum(jnp.where(same, row, 0.0), axis=1, keepdims=True)

    for load in small_loads[:3]:
        load.wait()
    shift = shift_ref[...].reshape(1, D)
    scale = 1.0 + scale_ref[...].reshape(1, D)

    def modulate(first, count):
        for block in range(count // NORM_BLOCK):
            rows = pl.ds(first + block * NORM_BLOCK, NORM_BLOCK)
            values = tokens[rows, :].astype(F32)
            center = values - jnp.mean(values, axis=-1, keepdims=True)
            spread = jnp.mean(center * center, axis=-1, keepdims=True)
            normed = center * (1.0 / jnp.sqrt(spread + EPSILON))
            hidden[rows, :] = (normed * scale + shift).astype(BF16)

    def project(part):
        for block in range(D // BLOCK):
            columns = pl.ds(block * BLOCK, BLOCK)
            fresh = dot(hidden[...], weight[part, :, columns]).astype(BF16)
            mask = own_mask[...]
            mask = jnp.concatenate([mask] * (BLOCK // 128), axis=1)
            old = stale[part - 1, :, columns].astype(F32)
            fresh = jnp.where(mask > 0.5, fresh.astype(F32), old).astype(BF16)
            turned[columns, :] = fresh.T

    def head_norm(values, gain):
        values = values.astype(F32)
        mean = jnp.sum(values * values, axis=0, keepdims=True) * (1.0 / HD)
        return (values * (1.0 / jnp.sqrt(mean + EPSILON)) * gain).astype(BF16)

    def query_copy(part, k):
        return pltpu.make_async_remote_copy(
            src_ref=query_send.at[part, target(k)],
            dst_ref=query_recv.at[part, me],
            send_sem=q_send_sem,
            recv_sem=q_recv_sem.at[k],
            device_id=(grp, target(k)),
            device_id_type=MESH,
        )

    def kv_copy(head, k):
        return pltpu.make_async_remote_copy(
            src_ref=kv_send.at[head, target(k)],
            dst_ref=kv_recv.at[head, me],
            send_sem=kv_send_sem,
            recv_sem=kv_recv_sem.at[head, STEP_OF[k]],
            device_id=(grp, target(k)),
            device_id_type=MESH,
        )

    def out_copy(head, k):
        return pltpu.make_async_remote_copy(
            src_ref=out_send.at[head, target(k)],
            dst_ref=out_recv.at[me, head],
            send_sem=o_send_sem,
            recv_sem=o_recv_sem,
            device_id=(grp, target(k)),
            device_id_type=MESH,
        )

    def own_out(head):
        return pltpu.make_async_copy(out_send.at[head, me], out_recv.at[me, head], own_sem)

    def wait_bytes(ref, sem):
        pltpu.make_async_copy(ref, ref, sem).wait()

    gain = column(query_gain_ref)
    for part in range(QUERY_PARTS):
        with jax.named_scope("norm"):
            loads[part].wait()
            modulate(part * QUERY_ROWS, QUERY_ROWS)
        with jax.named_scope("proj_q"):
            if part == 0:
                weight_loads[0].wait()
            rows = pl.ds(part * QUERY_ROWS, QUERY_ROWS)
            for block in range(D // BLOCK):
                columns = pl.ds(block * BLOCK, BLOCK)
                fresh = dot(hidden[rows, :], weight[0, :, columns]).astype(BF16)
                turned[columns, rows] = fresh.T
        with jax.named_scope("norm_q"):
            for head in range(H):
                query_send[part, head // HEADS_DEV, head % HEADS_DEV] = head_norm(
                    turned[pl.ds(head * HD, HD), rows], gain
                )
        if part == 0:
            with jax.named_scope("barrier"):
                pl.semaphore_wait(barrier, PARTS - 1)
        for k in range(PARTS - 1):
            query_copy(part, k).start()

    for load in small_loads[3:]:
        load.wait()
    flags = refreshed_ref[...].reshape(1, TILES).astype(F32)
    tile_row = lax.broadcasted_iota(jnp.int32, (TILES, TILES), 0)
    tile_col = lax.broadcasted_iota(jnp.int32, (TILES, TILES), 1)
    flag_rows = jnp.broadcast_to(flags, (TILES, TILES))
    until = jnp.where(tile_col <= tile_row, flag_rows, 0.0).astype(BF16)
    inclusive = dot(until, jnp.ones((TILES, 128), BF16))
    slots = lax.broadcasted_iota(jnp.int32, (TILES, 128), 1).astype(F32)
    which = jnp.sum(jnp.where(inclusive <= slots, 1.0, 0.0), axis=0, keepdims=True)
    which = jnp.minimum(which, float(TILES - 1))
    before = jnp.where(tile_row < tile_col, 1.0, 0.0).astype(BF16)
    rank = dot(jnp.broadcast_to(flags, (8, TILES)).astype(BF16), before)[0:1]
    rank = jnp.minimum(rank, float(REFRESHED - 1))
    plan_vmem[0:1, 0:128] = which.astype(jnp.int32)
    plan_vmem[1:2, 0:TILES] = rank.astype(jnp.int32)
    plan_copy = pltpu.make_async_copy(plan_vmem, plan, plan_sem)
    plan_copy.start()
    row_tile = lax.broadcasted_iota(jnp.int32, (ROWS, TILES), 0) // TILE + me * TILES_DEV
    row_col = lax.broadcasted_iota(jnp.int32, (ROWS, TILES), 1)
    chosen = jnp.where(row_tile == row_col, jnp.broadcast_to(flags, (ROWS, TILES)), 0.0)
    own_mask[...] = dot(chosen.astype(BF16), jnp.ones((TILES, 128), BF16))

    with jax.named_scope("proj_k"):
        weight_loads[1].wait()
        stale_loads[0].wait()
        project(1)
    with jax.named_scope("norm_k"):
        gain = column(key_gain_ref)
        for head in range(H):
            values = turned[pl.ds(head * HD, HD), :]
            kv_send[head % HEADS_DEV, head // HEADS_DEV, 0] = head_norm(values, gain)
    with jax.named_scope("proj_v"):
        weight_loads[2].wait()
        stale_loads[1].wait()
        project(2)
    with jax.named_scope("put_v"):
        for head in range(H):
            kv_send[head % HEADS_DEV, head // HEADS_DEV, 1] = turned[pl.ds(head * HD, HD), :]
    for h in range(HEADS_DEV):
        for k in range(PARTS - 1):
            kv_copy(h, k).start()

    numerator[...] = jnp.zeros_like(numerator)
    totals[...] = jnp.zeros_like(totals)
    same = eye(QUERY_ROWS)
    part_tiles = QUERY_ROWS // TILE

    def turn_queries(buffer, part, index):
        for h in range(HEADS_DEV):
            rows = dot_nt(same, buffer[part, index, h]).astype(BF16)
            tiles = pl.ds(index * TILES_DEV + part * part_tiles, part_tiles)
            query_rows[h, tiles] = rows.reshape(part_tiles, TILE, HD)

    with jax.named_scope("turn_q"):
        for part in range(QUERY_PARTS):
            turn_queries(query_send, part, me)
        for k in range(PARTS - 1):
            with jax.named_scope(f"wait_q#k={k}"):
                wait_bytes(query_recv.at[:, source(k)], q_recv_sem.at[k])
            for part in range(QUERY_PARTS):
                turn_queries(query_recv, part, source(k))
    with jax.named_scope("keep_fresh"):
        plan_copy.wait()
        for slot in range(REFRESHED):
            tile = jnp.clip(plan[0, slot], 0, TILES - 1)
            for h in range(HEADS_DEV):
                query_fresh[h, slot] = query_rows[h, tile]
    factor = math.log2(math.e) / math.sqrt(HD)
    tiles_block = QBLOCK // TILE

    def add_blocks(head, blocks):
        keys = jnp.concatenate([ref[head, index, 0] for ref, index in blocks], axis=1)
        values = jnp.concatenate([ref[head, index, 1] for ref, index in blocks], axis=1)
        for block in range(FRESH // QBLOCK):
            rows = pl.ds(block * QBLOCK, QBLOCK)
            queries = query_fresh[head, pl.ds(block * tiles_block, tiles_block)]
            scores = dot(queries.reshape(QBLOCK, HD), keys)
            weights = jnp.exp2(scores * factor)
            sums = weights[:, 0:128]
            for lane in range(128, ROWS * len(blocks), 128):
                sums = sums + weights[:, lane : lane + 128]
            totals[head, rows, :] += sums
            numerator[head, rows, :] += dot_nt(weights.astype(BF16), values)

    def send_out(head):
        for block in range(FRESH // QBLOCK):
            rows = pl.ds(block * QBLOCK, QBLOCK)
            total = jnp.sum(totals[head, rows, :], axis=1, keepdims=True)
            result = (numerator[head, rows, :] / total).astype(BF16)
            attended[head, pl.ds(block * tiles_block, tiles_block)] = result.reshape(
                tiles_block, TILE, HD
            )

        same = eye(HD)
        for group in ((0, 1, 2, 3), (4, 5, 6, 7)):
            for k in group:
                owner = target(k) if k < PARTS - 1 else me
                pieces = []
                for tile in range(TILES_DEV):
                    item = jnp.clip(plan[1, owner * TILES_DEV + tile], 0, REFRESHED - 1)
                    pieces.append(attended[head, item])
                rows = jnp.concatenate(pieces, axis=0)
                out_send[head, owner] = dot_nt(same, rows).astype(BF16)
            for k in group:
                if k < PARTS - 1:
                    out_copy(head, k).start()
        own_out(head).start()

    for h, step in STEPS:
        with jax.named_scope(f"wait_kv#h={h}#k={step[0]}"):
            wait_bytes(kv_recv.at[h, pl.ds(0, len(step))], kv_recv_sem.at[h, STEP_OF[step[0]]])
        with jax.named_scope("add"):
            blocks = [(kv_recv, source(k)) for k in step]
            if len(step) == 1:
                blocks.append((kv_send, me))
            add_blocks(h, blocks)
        if step == STEPS[-1][1]:
            with jax.named_scope("send_out"):
                send_out(h)

    with jax.named_scope("wait_out"):
        stale_loads[2].wait()
        wait_bytes(out_recv.at[me], own_sem)
        wait_bytes(out_recv.at[pl.ds(0, PARTS - 1)], o_recv_sem)
    with jax.named_scope("merge"):
        mask = own_mask[...] > 0.5
        for block in range(D // 128):
            columns = pl.ds(block * 128, 128)
            heads = range(block * 128 // HD, (block * 128 + 127) // HD + 1)
            for head in heads:
                if head * HD >= block * 128 or block == 0:
                    turned[pl.ds(head * HD, HD), :] = out_recv[head // HEADS_DEV, head % HEADS_DEV]
            fresh = turned[columns, :].T.astype(F32)
            old = stale[2, :, columns].astype(F32)
            result[:, columns] = jnp.where(mask, fresh, old).astype(BF16)
            if block % 3 == 2:
                columns = pl.ds((block - 2) * 128, 3 * 128)
                pltpu.make_async_copy(
                    result.at[:, columns], out_hbm.at[:, columns], store_sem
                ).start()
    with jax.named_scope("wait_end"):
        wait_bytes(query_send.at[:, pl.ds(0, PARTS - 1)], q_send_sem)
        wait_bytes(kv_send.at[:, pl.ds(0, PARTS - 1)], kv_send_sem)
        wait_bytes(out_send.at[:, pl.ds(0, PARTS - 1)], o_send_sem)
        pltpu.make_async_copy(result, out_hbm, store_sem).wait()


def step(
    tokens,
    projection_weight,
    shift_term,
    scale_term,
    query_gain,
    key_gain,
    stale_keys,
    stale_values,
    stale_output,
    refreshed,
):
    hbm = pl.BlockSpec(memory_space=pltpu.HBM)
    dma = pltpu.SemaphoreType.DMA
    others = PARTS - 1
    scratch = [
        pltpu.VMEM((D,), F32),
        pltpu.VMEM((D,), F32),
        pltpu.VMEM((HD,), F32),
        pltpu.VMEM((HD,), F32),
        pltpu.VMEM((TILES,), jnp.int32),
        pltpu.VMEM((ROWS, D), BF16),
        pltpu.VMEM((3, D, D), BF16),
        pltpu.VMEM((3, ROWS, D), BF16),
        pltpu.VMEM((ROWS, D), BF16),
        pltpu.VMEM((D, ROWS), BF16),
        pltpu.VMEM((ROWS, 128), F32),
        pltpu.VMEM((QUERY_PARTS, PARTS, HEADS_DEV, HD, QUERY_ROWS), BF16),
        pltpu.VMEM((HEADS_DEV, PARTS, 2, HD, ROWS), BF16),
        pltpu.VMEM((QUERY_PARTS, PARTS, HEADS_DEV, HD, QUERY_ROWS), BF16),
        pltpu.VMEM((HEADS_DEV, PARTS, 2, HD, ROWS), BF16),
        pltpu.VMEM((HEADS_DEV, TILES, TILE, HD), BF16),
        pltpu.VMEM((HEADS_DEV, REFRESHED, TILE, HD), BF16),
        pltpu.VMEM((HEADS_DEV, FRESH, HD), F32),
        pltpu.VMEM((HEADS_DEV, FRESH, 128), F32),
        pltpu.VMEM((HEADS_DEV, REFRESHED, TILE, HD), BF16),
        pltpu.VMEM((HEADS_DEV, PARTS, HD, ROWS), BF16),
        pltpu.VMEM((PARTS, HEADS_DEV, HD, ROWS), BF16),
        pltpu.VMEM((ROWS, D), BF16),
        pltpu.VMEM((2, 256), jnp.int32),
        pltpu.SMEM((2, 256), jnp.int32),
        dma((5,)),
        dma((QUERY_PARTS,)),
        dma((3,)),
        dma((3,)),
        dma,
        dma,
        dma,
        dma,
        dma((others,)),
        dma,
        dma((HEADS_DEV, 4)),
        dma,
        dma,
    ]
    return pl.pallas_call(
        kernel,
        out_shape=jax.ShapeDtypeStruct((ROWS, D), BF16),
        in_specs=[hbm] * 10,
        out_specs=hbm,
        scratch_shapes=scratch,
        compiler_params=pltpu.CompilerParams(
            collective_id=0, has_side_effects=True, vmem_limit_bytes=63 * 2**20
        ),
    )(
        tokens,
        projection_weight,
        shift_term,
        scale_term,
        query_gain,
        key_gain,
        stale_keys,
        stale_values,
        stale_output,
        refreshed,
    )


def solution(mesh):
    rows = P(("grp", "patch"), None)
    in_specs = (rows, P(), P(), P(), P(), P(), rows, rows, rows, P("grp"))
    return jax.shard_map(step, mesh=mesh, in_specs=in_specs, out_specs=rows, check_vma=False)
```
